16 devices in a mesh: dp: 1, tp: 16 (over x, y, z, core).
Axes of the slice: x: 2, y: 2, z: 2, core: 2. Of those that a mesh axis runs over, the one named last changes fastest.
Arguments:
- x: bfloat16 [2560, 7168], P(('dp', 'tp'))
- dy: bfloat16 [2560, 7168], P(('dp', 'tp'))
- gate: bfloat16 [2560, 20480], P('dp', 'tp')
- up: bfloat16 [2560, 20480], P('dp', 'tp')
- w_gate: bfloat16 [7168, 20480], P(None, 'tp')
- w_up: bfloat16 [7168, 20480], P(None, 'tp')
- w_down: bfloat16 [20480, 7168], P('tp')
Outputs:
- output 1: bfloat16 [2560, 7168], P(('dp', 'tp'))
- output 2: bfloat16 [7168, 20480], P('dp', 'tp')
- output 3: bfloat16 [7168, 20480], P('dp', 'tp')
- output 4: bfloat16 [20480, 7168], P(('dp', 'tp'))
All inputs are finite; a program needn't handle non-finite values.
Results may differ from the reference program's by a relative error of at most 0.012.
Values are sent between devices in bfloat16 or wider.
A program may use at most 2 GiB of HBM per device.

```python
import jax
import jax.numpy as jnp

ROWS = 2560
D = 7168
FF = 20480


def act(gate, up):
    return jax.nn.silu(gate) * up


def setup_inputs(seed: int = 0, part: int = 0) -> dict:
    kx, ky, ka, kb, kg, ku, kd = jax.random.split(jax.random.key(seed), 7)
    kx, ky, ka, kb = (jax.random.fold_in(k, part) for k in (kx, ky, ka, kb))
    drawn = {
        "x": jax.random.normal(kx, (ROWS, D), jnp.float32),
        "dy": jax.random.normal(ky, (ROWS, D), jnp.float32),
        "gate": jax.random.normal(ka, (ROWS, FF), jnp.float32),
        "up": jax.random.normal(kb, (ROWS, FF), jnp.float32),
        "w_gate": jax.random.normal(kg, (D, FF), jnp.float32) * D**-0.5,
        "w_up": jax.random.normal(ku, (D, FF), jnp.float32) * D**-0.5,
        "w_down": jax.random.normal(kd, (FF, D), jnp.float32) * FF**-0.5,
    }
    return {k: v.astype(jnp.bfloat16) for k, v in drawn.items()}


def reference(x, dy, gate, up, w_gate, w_up, w_down):
    hidden, back = jax.vjp(act, gate.astype(jnp.float32), up.astype(jnp.float32))
    d_hidden = jnp.dot(dy, w_down.T, preferred_element_type=jnp.float32)
    d_gate, d_up = (g.astype(jnp.bfloat16) for g in back(d_hidden))
    dx = jnp.dot(d_gate, w_gate.T, preferred_element_type=jnp.float32) + jnp.dot(d_up, w_up.T, preferred_element_type=jnp.float32)
    dw_gate = jnp.dot(x.T, d_gate, preferred_element_type=jnp.float32)
    dw_up = jnp.dot(x.T, d_up, preferred_element_type=jnp.float32)
    dw_down = jnp.dot(hidden.astype(jnp.bfloat16).T, dy, preferred_element_type=jnp.float32)
    return tuple(g.astype(jnp.bfloat16) for g in (dx, dw_gate, dw_up, dw_down))
```

```python
import functools
import jax
import jax.numpy as jnp
from jax import lax
from jax.experimental import pallas as pl
from jax.experimental.pallas import tpu as pltpu
from jax.sharding import PartitionSpec as P

F32, BF16 = jnp.float32, jnp.bfloat16
NT = (((1,), (1,)), ((), ()))
TN = (((0,), (0,)), ((), ()))
L1, L2, L3 = 3, 2, 2
LAG = 1 + L1 + L2 + L3
OWN, SIB, SND = LAG + 1, LAG + 2, 3


def weight(j):
    return (8 - 5 * j + j * j) // 2


def flip(i, w):
    return i + w - 2 * w * ((i // w) % 2)


def rs_kernel(tiles, dg_hbm, du_hbm, wg_hbm, wu_hbm, dx_ref, dg, w, own, sib, s0, s1, r1, s2, r2, s3, r3,
              dg_sem, w_sem, s0_sem, sib_sem, s1_sem, r1_sem, s2_sem, r2_sem, s3_sem, r3_sem, free_sem):
    me = lax.axis_index("tp")
    chip, core = me // 2, me % 2
    rows, k = dg.shape[2], dg_hbm.shape[1]
    ct = w.shape[1]

    def dev(i):
        return {"tp": i}

    barrier = pltpu.get_barrier_semaphore()
    for m in (1, 2, 4, 8):
        pl.semaphore_signal(barrier, inc=1, device_id=dev(flip(me, m)), device_id_type=pl.DeviceIdType.MESH)

    def load_block(c, r, half, src):
        other = (core + 1 - c) % 2
        target = chip
        for wt in (4, 2, 1):
            if r & wt:
                target = flip(target, wt)
        return pltpu.make_async_copy(
            src.at[pl.ds((target * 2 + other) * rows, rows)],
            dg.at[c, r, :, pl.ds(half * k, k)],
            dg_sem.at[(c * 8 + r) * 2 + half],
        )

    blocks = [load_block(c, r, h, s) for c in range(2) for r in range(8) for h, s in ((0, dg_hbm), (1, du_hbm))]

    def load_w(t, slot):
        return [
            pltpu.make_async_copy(s.at[pl.ds(t * ct, ct)], w.at[slot, :, pl.ds(h * k, k)], w_sem.at[slot, h])
            for h, s in ((0, wg_hbm), (1, wu_hbm))
        ]

    for c in load_w(0, 0):
        c.start()
    for b in blocks:
        b.start()
    for b in blocks:
        b.wait()
    pl.semaphore_wait(barrier, 4)

    def remote(src, dst, ssem, rsem, to):
        return pltpu.make_async_remote_copy(
            src_ref=src, dst_ref=dst, send_sem=ssem, recv_sem=rsem, device_id=dev(to),
            device_id_type=pl.DeviceIdType.MESH)

    def c0(t):
        return remote(s0.at[t % SND], sib.at[t % SIB], s0_sem.at[t % SND], sib_sem.at[t % SIB], flip(me, 1))

    def axes(t):
        j = t % 3
        return weight(j), weight((j + 1) % 3), weight((j + 2) % 3)

    def c1(t):
        return remote(s1.at[t % SND], r1.at[t], s1_sem.at[t % SND], r1_sem.at[t], flip(me, 2 * axes(t)[0]))

    def c2(t):
        return remote(s2.at[t % SND], r2.at[t], s2_sem.at[t % SND], r2_sem.at[t], flip(me, 2 * axes(t)[1]))

    def c3(t):
        return remote(s3.at[t % SND], r3.at[t], s3_sem.at[t % SND], r3_sem.at[t], flip(me, 2 * axes(t)[2]))

    def base(t, r):
        return own[t % OWN, r] + sib[t % SIB, r].astype(F32)

    def when(cond, f):
        pl.when(cond)(f)

    def step(i, _):
        slot = i % 2

        @pl.when(i < tiles)
        def _():
            @pl.when(i + 1 < tiles)
            def _():
                for c in load_w(i + 1, (i + 1) % 2):
                    c.start()
            for c in load_w(i, slot):
                c.wait()
            @pl.when(i >= SND)
            def _():
                c0(i - SND).wait_send()
            part = lax.dot_general(dg[0].reshape(8 * rows, 2 * k), w[slot], NT, preferred_element_type=F32)
            s0[i % SND] = part.astype(BF16).reshape(8, rows, ct)

        t = i - 1

        @pl.when((t >= 0) & (t < tiles))
        def _():
            @pl.when(t >= SND)
            def _():
                c1(t - SND).wait_send()
            c0(t).wait_recv()
            a, b, c = axes(t)
            for q, r in enumerate((a, a + c, a + b, a + b + c)):
                s1[t % SND, q] = base(t, r).astype(BF16)

        t2 = i - 1 - L1

        @pl.when((t2 >= 0) & (t2 < tiles))
        def _():
            @pl.when(t2 >= SND)
            def _():
                c2(t2 - SND).wait_send()
            c1(t2).wait_recv()
            a, b, c = axes(t2)
            for q, r in enumerate((b, b + c)):
                s2[t2 % SND, q] = (base(t2, r) + r1[t2, 2 + q].astype(F32)).astype(BF16)

        t3 = i - 1 - L1 - L2

        @pl.when((t3 >= 0) & (t3 < tiles))
        def _():
            @pl.when(t3 >= SND)
            def _():
                c3(t3 - SND).wait_send()
            c2(t3).wait_recv()
            a, b, c = axes(t3)
            s3[t3 % SND] = (base(t3, c) + r1[t3, 1].astype(F32) + r2[t3, 1].astype(F32)).astype(BF16)

        t4 = i - LAG

        @pl.when((t4 >= 0) & (t4 < tiles))
        def _():
            c3(t4).wait_recv()
            total = base(t4, 0) + r1[t4, 0].astype(F32) + r2[t4, 0].astype(F32) + r3[t4].astype(F32)
            dx_ref[:, pl.ds(pl.multiple_of(t4 * ct, ct), ct)] = total.astype(BF16)

            @pl.when(t4 < tiles - SIB)
            def _():
                pl.semaphore_signal(free_sem, inc=1, device_id=dev(flip(me, 1)), device_id_type=pl.DeviceIdType.MESH)

        @pl.when(i < tiles)
        def _():
            @pl.when(i >= SIB)
            def _():
                pl.semaphore_wait(free_sem, 1)
            c0(i).start()

        @pl.when((t >= 0) & (t < tiles))
        def _():
            c1(t).start()

        @pl.when((t2 >= 0) & (t2 < tiles))
        def _():
            c2(t2).start()

        @pl.when((t3 >= 0) & (t3 < tiles))
        def _():
            c3(t3).start()

        @pl.when(i < tiles)
        def _():
            part = lax.dot_general(dg[1].reshape(8 * rows, 2 * k), w[slot], NT, preferred_element_type=F32)
            own[i % OWN] = part.reshape(8, rows, ct)
        return 0

    lax.fori_loop(0, tiles + LAG, step, 0)
    for t in range(tiles - SND, tiles):
        for c in (c0, c1, c2, c3):
            c(t).wait_send()


def dx_reduce_scatter(d_gate, d_up, w_gate, w_up, ct=256):
    n, k = d_gate.shape
    d = w_gate.shape[0]
    rows, tiles = n // 16, d // ct
    any_ = pl.BlockSpec(memory_space=pl.ANY)
    dma = pltpu.SemaphoreType.DMA
    v = pltpu.VMEM
    return pl.pallas_call(
        functools.partial(rs_kernel, tiles),
        out_shape=jax.ShapeDtypeStruct((rows, d), BF16),
        in_specs=[any_] * 4,
        out_specs=pl.BlockSpec(memory_space=pltpu.VMEM),
        scratch_shapes=[
            v((2, 8, rows, 2 * k), BF16), v((2, ct, 2 * k), BF16), v((OWN, 8, rows, ct), F32),
            v((SIB, 8, rows, ct), BF16), v((SND, 8, rows, ct), BF16),
            v((SND, 4, rows, ct), BF16), v((tiles, 4, rows, ct), BF16),
            v((SND, 2, rows, ct), BF16), v((tiles, 2, rows, ct), BF16),
            v((SND, rows, ct), BF16), v((tiles, rows, ct), BF16),
            dma((32,)), dma((2, 2)), dma((SND,)), dma((SIB,)), dma((SND,)), dma((tiles,)),
            dma((SND,)), dma((tiles,)), dma((SND,)), dma((tiles,)), pltpu.SemaphoreType.REGULAR,
        ],
        compiler_params=pltpu.CompilerParams(collective_id=0, has_side_effects=True, vmem_limit_bytes=66000000),
        cost_estimate=pl.CostEstimate(flops=2 * n * k * d * 2, bytes_accessed=4 * n * k + 4 * k * d, transcendentals=0),
    )(d_gate, d_up, w_gate, w_up)


def act(gate, up):
    return jax.nn.silu(gate) * up


def solution(mesh):
    def body(x, dy, gate, up, w_gate, w_up, w_down):
        dy_all = lax.all_gather(dy, "tp", tiled=True)
        hidden, back = jax.vjp(act, gate.astype(F32), up.astype(F32))
        d_hidden = lax.dot_general(dy_all, w_down, NT, preferred_element_type=F32)
        d_gate, d_up = (g.astype(BF16) for g in back(d_hidden))
        dx = dx_reduce_scatter(d_gate, d_up, w_gate, w_up)
        x_all = lax.all_gather(x, "tp", tiled=True)
        dw_gate = lax.dot_general(x_all, d_gate, TN, preferred_element_type=F32).astype(BF16)
        dw_up = lax.dot_general(x_all, d_up, TN, preferred_element_type=F32).astype(BF16)
        dw_down = lax.dot_general(hidden.astype(BF16), dy_all, TN, preferred_element_type=F32).astype(BF16)
        return dx, dw_gate, dw_up, dw_down

    rows, cols = P(("dp", "tp"), None), P("dp", "tp")
    return jax.shard_map(
        body,
        mesh=mesh,
        in_specs=(rows, rows, cols, cols, P(None, "tp"), P(None, "tp"), P("tp", None)),
        out_specs=(rows, cols, cols, P(("dp", "tp"), None)),
        check_vma=False,
    )
```

```python
import functools

import jax
import jax.numpy as jnp
from jax import lax
from jax.experimental import pallas as pl
from jax.experimental.pallas import tpu as pltpu
from jax.sharding import PartitionSpec as P

F32, BF16 = jnp.float32, jnp.bfloat16
NT = (((1,), (1,)), ((), ()))
TN = (((0,), (0,)), ((), ()))
MESH = pl.DeviceIdType.MESH

A1, A2, A3 = 2, 2, 3
LAG_A = A1 + A2 + A3 + 1
B1, B2, B3 = 3, 2, 2
LAG_B = 1 + B1 + B2 + B3
NS = 10
NR = 10
SND = 3


def weight(j):
    return (8 - 5 * j + j * j) // 2


def flip(i, w):
    return i + w - 2 * w * ((i // w) % 2)


def axes(t):
    j = t % 3
    return weight(j), weight((j + 1) % 3), weight((j + 2) % 3)


def remote(src, dst, ssem, rsem, to):
    return pltpu.make_async_remote_copy(
        src_ref=src, dst_ref=dst, send_sem=ssem, recv_sem=rsem, device_id={"tp": to}, device_id_type=MESH
    )


def kernel(
    tiles, x_hbm, dy_hbm, gate_hbm, up_hbm, wg_hbm, wu_hbm, wd_hbm, dx_ref, dwg_hbm, dwu_hbm, dwd_hbm,
    ag, acc, hid, dg, w, wd, dwd, s0, s1, s2, s3, r1, r2, r3,
    ag_send, ag_recv, own_sem, load_sem, w_sem, wd_sem, dwd_sem, out_sem,
    s0_sem, s1_sem, s2_sem, s3_sem, r0_sem, r1_sem, r2_sem, r3_sem, credit_a, credit_b,
):
    me = lax.axis_index("tp")
    chip, core = me // 2, me % 2
    rows, ct = s3.shape[1], s3.shape[2]
    ff = gate_hbm.shape[1]
    nf = ff // ct
    half = 8 * rows
    peers = [flip(me, m) for m in (1, 2, 4, 8)]

    barrier = pltpu.get_barrier_semaphore()
    for p in peers:
        pl.semaphore_signal(barrier, inc=1, device_id={"tp": p}, device_id_type=MESH)

    def give(sem, n=1):
        for m, p in enumerate(peers):
            pl.semaphore_signal(sem.at[m], inc=n, device_id={"tp": p}, device_id_type=MESH)

    def take(sem):
        for m in range(4):
            pl.semaphore_wait(sem.at[m], 1)

    def load_rows(b, h):
        c, r = b // 8, b % 8
        target = chip
        for wt in (4, 2, 1):
            target = target + wt * ((r // wt) % 2) * (1 - 2 * ((chip // wt) % 2))
        src = (gate_hbm, up_hbm)[h]
        return pltpu.make_async_copy(
            src.at[pl.ds((target * 2 + (core + 1 - c) % 2) * rows, rows)],
            dg.at[c, r, :, pl.ds(h * ff, ff)],
            load_sem.at[b, h],
        )

    def cols(t):
        return pl.ds(pl.multiple_of(t * ct, ct), ct)

    def own_load(src, t, slot):
        return pltpu.make_async_copy(src.at[:, cols(t)], ag.at[slot, 1, 0], own_sem.at[slot])

    def hop(slot, q, m):
        return remote(
            ag.at[slot, 1, q], ag.at[slot, 1, q + m], ag_send.at[slot, q + m], ag_recv.at[slot, q + m], flip(me, 2 * m)
        )

    def share(slot):
        return remote(ag.at[slot, 1], ag.at[slot, 0], ag_send.at[slot, 0], ag_recv.at[slot, 0], flip(me, 1))

    def gather_step(src, first, i):
        @pl.when((i >= 0) & (i < tiles))
        def _():
            g = i + first
            slot = g % NS
            own_load(src, i, slot).wait()

            @pl.when(g >= NS)
            def _():
                take(credit_a)

            hop(slot, 0, axes(g)[0]).start()

            @pl.when(i + 1 < tiles)
            def _():
                own_load(src, i + 1, (g + 1) % NS).start()

        t2 = i - A1

        @pl.when((t2 >= 0) & (t2 < tiles))
        def _():
            g = t2 + first
            slot = g % NS
            a, b, c = axes(g)
            hop(slot, 0, a).wait_recv()
            hop(slot, 0, b).start()
            hop(slot, a, b).start()

        t3 = i - A1 - A2

        @pl.when((t3 >= 0) & (t3 < tiles))
        def _():
            g = t3 + first
            slot = g % NS
            a, b, c = axes(g)
            hop(slot, 0, b).wait_recv()
            hop(slot, a, b).wait_recv()
            for q in (0, a, b, a + b):
                hop(slot, q, c).start()

        t4 = i - A1 - A2 - A3

        @pl.when((t4 >= 0) & (t4 < tiles))
        def _():
            g = t4 + first
            slot = g % NS
            a, b, c = axes(g)
            for q in (0, a, b, a + b):
                hop(slot, q, c).wait_recv()
            share(slot).start()

    def release(g, last):
        slot = g % NS
        a, b, c = axes(g)
        hop(slot, 0, a).wait_send()
        for q in (0, a):
            hop(slot, q, b).wait_send()
        for q in (0, a, b, a + b):
            hop(slot, q, c).wait_send()
        share(slot).wait_send()

        @pl.when(g < last)
        def _():
            give(credit_a)

    def load_wd(t):
        return pltpu.make_async_copy(wd_hbm.at[:, cols(t)], wd.at[t % 2], wd_sem.at[t % 2])

    def load_w(t):
        return [
            pltpu.make_async_copy(
                s.at[pl.ds(pl.multiple_of(t * ct, ct), ct)], w.at[t % 2, :, pl.ds(h * ff, ff)], w_sem.at[t % 2, h]
            )
            for h, s in ((0, wg_hbm), (1, wu_hbm))
        ]

    def store_dwd(t):
        return pltpu.make_async_copy(dwd.at[t % 2], dwd_hbm.at[:, cols(t)], dwd_sem.at[t % 2])

    own_load(dy_hbm, 0, 0).start()

    def start_rows(b, _):
        load_rows(b, 0).start()
        load_rows(b, 1).start()
        return 0

    lax.fori_loop(0, 16, start_rows, 0)
    load_wd(0).start()
    pl.semaphore_wait(barrier, 4)

    def hidden_block(b):
        c, r = b // 8, b % 8
        load_rows(b, 0).wait()
        load_rows(b, 1).wait()
        for n in range(nf):
            g = dg[c, r, :, n * ct : (n + 1) * ct].astype(F32)
            u = dg[c, r, :, ff + n * ct : ff + (n + 1) * ct].astype(F32)
            hid[pl.ds(pl.multiple_of(b * rows, rows), rows), n * ct : (n + 1) * ct] = (g * jax.nn.sigmoid(g) * u).astype(BF16)
            acc[c, r, :, n * ct : (n + 1) * ct] = jnp.zeros((rows, ct), F32)

    def fill(i, _):
        gather_step(dy_hbm, 0, i)
        per = 16 // LAG_A
        for e in range(per):
            hidden_block(i * per + e)
        return 0

    lax.fori_loop(0, LAG_A, fill, 0)

    def step_a(t, _):
        gather_step(dy_hbm, 0, t + LAG_A)
        slot = t % NS

        @pl.when(t + 1 < tiles)
        def _():
            load_wd(t + 1).start()

        load_wd(t).wait()
        share(slot).wait_recv()
        for c in range(2):
            block = ag[slot, c].reshape(half, ct)
            for n in range(nf):
                part = lax.dot_general(
                    block, wd[t % 2, n * ct : (n + 1) * ct, :], NT, preferred_element_type=F32
                )
                acc[c, :, :, n * ct : (n + 1) * ct] += part.reshape(8, rows, ct)

        @pl.when(t >= 2)
        def _():
            store_dwd(t - 2).wait()

        for n in range(nf):
            dwd[t % 2, n * ct : (n + 1) * ct, :] = lax.dot_general(
                hid[:, n * ct : (n + 1) * ct], ag[slot].reshape(2 * half, ct), TN, preferred_element_type=F32
            ).astype(BF16)
        release(t, 2 * tiles - NS)
        store_dwd(t).start()
        return 0

    lax.fori_loop(0, tiles, step_a, 0)

    give(credit_b, NR)
    for c in load_w(0):
        c.start()
    own_load(x_hbm, 0, tiles % NS).start()

    def d_act(b, _):
        @pl.when(b % 4 == 0)
        def _():
            gather_step(x_hbm, tiles, b // 4)

        c, r = b // 8, b % 8
        for n in range(nf):
            lo, hi = slice(n * ct, (n + 1) * ct), slice(ff + n * ct, ff + (n + 1) * ct)
            g, u, d = dg[c, r, :, lo].astype(F32), dg[c, r, :, hi].astype(F32), acc[c, r, :, lo]
            s = jax.nn.sigmoid(g)
            dg[c, r, :, lo] = (d * u * (s + g * s * (1.0 - s))).astype(BF16)
            dg[c, r, :, hi] = (d * (g * s)).astype(BF16)
        return 0

    lax.fori_loop(0, 16, d_act, 0)
    for t in (tiles - 2, tiles - 1):
        store_dwd(t).wait()

    def place(t):
        k = t % NR
        return k // nf, pl.ds(pl.multiple_of((k % nf) * ct, ct), ct)

    def c0(t):
        c, n = place(t)
        return remote(s0.at[t % SND], hid.at[pl.ds(pl.multiple_of(c * half, half), half), n], s0_sem.at[t % SND], r0_sem.at[t % NR], flip(me, 1))

    def c1(t):
        return remote(
            s1.at[t % SND], r1.at[t % NR], s1_sem.at[t % SND], r1_sem.at[t % NR], flip(me, 2 * axes(t)[0])
        )

    def c2(t):
        return remote(
            s2.at[t % SND], r2.at[t % NR], s2_sem.at[t % SND], r2_sem.at[t % NR], flip(me, 2 * axes(t)[1])
        )

    def c3(t):
        return remote(
            s3.at[t % SND], r3.at[t % NR], s3_sem.at[t % SND], r3_sem.at[t % NR], flip(me, 2 * axes(t)[2])
        )

    def chip_sum(t, r):
        c, n = place(t)
        return acc[c, r, :, n] + hid[pl.ds(pl.multiple_of(c * half + r * rows, rows), rows), n].astype(F32)

    def store_dw(t):
        return [
            pltpu.make_async_copy(
                w.at[t % 2, :, pl.ds(h * ff, ff)], o.at[pl.ds(pl.multiple_of(t * ct, ct), ct)], out_sem.at[t % 2, h]
            )
            for h, o in ((0, dwg_hbm), (1, dwu_hbm))
        ]

    def step_b(i, _):
        @pl.when(i < tiles)
        def _():
            @pl.when(i + 1 < tiles)
            def _():
                for c in load_w(i + 1):
                    c.start()

            for c in load_w(i):
                c.wait()

            @pl.when(i >= SND)
            def _():
                c0(i - SND).wait_send()

            part = lax.dot_general(dg[0].reshape(half, 2 * ff), w[i % 2], NT, preferred_element_type=F32)
            s0[i % SND] = part.astype(BF16)

        t1, t2, t3, t4 = i - 1, i - 1 - B1, i - 1 - B1 - B2, i - LAG_B

        @pl.when((t1 >= 0) & (t1 < tiles))
        def _():
            @pl.when(t1 >= SND)
            def _():
                c1(t1 - SND).wait_send()

            c0(t1).wait_recv()
            a, b, c = axes(t1)
            for q, r in enumerate((a, a + c, a + b, a + b + c)):
                s1[t1 % SND, q] = chip_sum(t1, r).astype(BF16)

        @pl.when((t2 >= 0) & (t2 < tiles))
        def _():
            @pl.when(t2 >= SND)
            def _():
                c2(t2 - SND).wait_send()

            c1(t2).wait_recv()
            a, b, c = axes(t2)
            for q, r in enumerate((b, b + c)):
                s2[t2 % SND, q] = (chip_sum(t2, r) + r1[t2 % NR, 2 + q].astype(F32)).astype(BF16)

        @pl.when((t3 >= 0) & (t3 < tiles))
        def _():
            @pl.when(t3 >= SND)
            def _():
                c3(t3 - SND).wait_send()

            c2(t3).wait_recv()
            a, b, c = axes(t3)
            s3[t3 % SND] = (
                chip_sum(t3, c) + r1[t3 % NR, 1].astype(F32) + r2[t3 % NR, 1].astype(F32)
            ).astype(BF16)

        @pl.when((t4 >= 0) & (t4 < tiles))
        def _():
            c3(t4).wait_recv()
            total = chip_sum(t4, 0) + r1[t4 % NR, 0].astype(F32) + r2[t4 % NR, 0].astype(F32)
            dx_ref[:, cols(t4)] = (total + r3[t4 % NR].astype(F32)).astype(BF16)

            @pl.when(t4 < tiles - NR)
            def _():
                give(credit_b)

        @pl.when(i < tiles)
        def _():
            take(credit_b)
            c0(i).start()

        for copy, t in ((c1, t1), (c2, t2), (c3, t3)):
            @pl.when((t >= 0) & (t < tiles))
            def _():
                copy(t).start()

        k = jnp.where(i < tiles, i + 4, i - tiles + LAG_A)

        @pl.when((i < LAG_A - 4) | (i >= tiles))
        def _():
            gather_step(x_hbm, tiles, k)

        @pl.when(i < tiles)
        def _():
            c, n = place(i)
            part = lax.dot_general(dg[1].reshape(half, 2 * ff), w[i % 2], NT, preferred_element_type=F32)
            acc[c, :, :, n] = part.reshape(8, rows, ct)

        t = i - tiles

        @pl.when(t >= 0)
        def _():
            g = t + tiles

            @pl.when(t >= 2)
            def _():
                for c in store_dw(t - 2):
                    c.wait()

            share(g % NS).wait_recv()
            block = ag[g % NS].reshape(2 * half, ct)
            for h in range(2):
                w[t % 2, :, h * ff : (h + 1) * ff] = lax.dot_general(
                    block, dg[:, :, :, h * ff : (h + 1) * ff].reshape(2 * half, ff), TN, preferred_element_type=F32
                ).astype(BF16)
            release(g, 2 * tiles - NS)
            for c in store_dw(t):
                c.start()

        return 0

    lax.fori_loop(0, 2 * tiles, step_b, 0)
    for t in range(tiles - SND, tiles):
        for c in (c0, c1, c2, c3):
            c(t).wait_send()
    for t in (tiles - 2, tiles - 1):
        for c in store_dw(t):
            c.wait()


def mlp_backward(x, dy, gate, up, w_gate, w_up, w_down, ct=256):
    rows, d = x.shape
    n, ff = gate.shape
    tiles, nf = d // ct, ff // ct
    assert n == 16 * rows and 2 * nf == NR and tiles >= NS
    anywhere = pl.BlockSpec(memory_space=pl.ANY)
    dma, vmem = pltpu.SemaphoreType.DMA, pltpu.VMEM
    return pl.pallas_call(
        functools.partial(kernel, tiles),
        out_shape=[
            jax.ShapeDtypeStruct((rows, d), BF16),
            jax.ShapeDtypeStruct((d, ff), BF16),
            jax.ShapeDtypeStruct((d, ff), BF16),
            jax.ShapeDtypeStruct((ff, d), BF16),
        ],
        in_specs=[anywhere] * 7,
        out_specs=[pl.BlockSpec(memory_space=vmem)] + [anywhere] * 3,
        scratch_shapes=[
            vmem((NS, 2, 8, rows, ct), BF16),
            vmem((2, 8, rows, ff), F32),
            vmem((16 * rows, ff), BF16),
            vmem((2, 8, rows, 2 * ff), BF16),
            vmem((2, ct, 2 * ff), BF16),
            vmem((2, ff, ct), BF16),
            vmem((2, ff, ct), BF16),
            vmem((SND, 8 * rows, ct), BF16),
            vmem((SND, 4, rows, ct), BF16),
            vmem((SND, 2, rows, ct), BF16),
            vmem((SND, rows, ct), BF16),
            vmem((NR, 4, rows, ct), BF16),
            vmem((NR, 2, rows, ct), BF16),
            vmem((NR, rows, ct), BF16),
            dma((NS, 8)), dma((NS, 8)), dma((NS,)), dma((16, 2)), dma((2, 2)), dma((2,)), dma((2,)), dma((2, 2)),
            dma((SND,)), dma((SND,)), dma((SND,)), dma((SND,)), dma((NR,)), dma((NR,)), dma((NR,)), dma((NR,)),
            pltpu.SemaphoreType.REGULAR((4,)), pltpu.SemaphoreType.REGULAR((4,)),
        ],
        compiler_params=pltpu.CompilerParams(collective_id=0, has_side_effects=True, vmem_limit_bytes=67000000),
        cost_estimate=pl.CostEstimate(flops=12 * n * ff * d, bytes_accessed=12 * ff * d, transcendentals=0),
    )(x, dy, gate, up, w_gate, w_up, w_down)


def solution(mesh):
    rows, cols = P(("dp", "tp"), None), P("dp", "tp")
    return jax.shard_map(
        mlp_backward,
        mesh=mesh,
        in_specs=(rows, rows, cols, cols, P(None, "tp"), P(None, "tp"), P("tp", None)),
        out_specs=(rows, cols, cols, P(("dp", "tp"), None)),
        check_vma=False,
    )
```

```python
import functools

import jax
import jax.numpy as jnp
from jax import lax
from jax.experimental import pallas as pl
from jax.experimental.pallas import tpu as pltpu
from jax.sharding import PartitionSpec as P

F32, BF16 = jnp.float32, jnp.bfloat16
NT = (((1,), (1,)), ((), ()))
TN = (((0,), (0,)), ((), ()))
MESH = pl.DeviceIdType.MESH

A1, A2, A3 = 2, 2, 3
LAG_A = A1 + A2 + A3 + 1
B1, B2, B3 = 3, 2, 2
LAG_B = 1 + B1 + B2 + B3
NS = 10
NR = 10
SND = 3


def weight(j):
    return (8 - 5 * j + j * j) // 2


def flip(i, w):
    return i + w - 2 * w * ((i // w) % 2)


def axes(t):
    j = t % 3
    return weight(j), weight((j + 1) % 3), weight((j + 2) % 3)


def remote(src, dst, ssem, rsem, to):
    return pltpu.make_async_remote_copy(
        src_ref=src, dst_ref=dst, send_sem=ssem, recv_sem=rsem, device_id={"tp": to}, device_id_type=MESH
    )


def kernel(
    tiles, x_hbm, dy_hbm, gate_hbm, up_hbm, wg_hbm, wu_hbm, wd_hbm, dx_ref, dwg_hbm, dwu_hbm, dwd_hbm,
    ag, acc, hid, dg, w, wd, dwd, s0, s1, s2, s3, r1, r2, r3,
    ag_send, ag_recv, own_sem, load_sem, w_sem, wd_sem, dwd_sem, out_sem,
    s0_sem, s1_sem, s2_sem, s3_sem, r0_sem, r1_sem, r2_sem, r3_sem, credit_a, credit_b,
):
    me = lax.axis_index("tp")
    chip, core = me // 2, me % 2
    rows, ct = s3.shape[1], s3.shape[2]
    ff = gate_hbm.shape[1]
    nf = ff // ct
    half = 8 * rows
    peers = [flip(me, m) for m in (1, 2, 4, 8)]

    barrier = pltpu.get_barrier_semaphore()
    for p in peers:
        pl.semaphore_signal(barrier, inc=1, device_id={"tp": p}, device_id_type=MESH)

    def give(sem, n=1):
        for m, p in enumerate(peers):
            pl.semaphore_signal(sem.at[m], inc=n, device_id={"tp": p}, device_id_type=MESH)

    def take(sem):
        for m in range(4):
            pl.semaphore_wait(sem.at[m], 1)

    def load_rows(b, h):
        c, r = b // 8, b % 8
        target = chip
        for wt in (4, 2, 1):
            target = target + wt * ((r // wt) % 2) * (1 - 2 * ((chip // wt) % 2))
        src = (gate_hbm, up_hbm)[h]
        return pltpu.make_async_copy(
            src.at[pl.ds((target * 2 + (core + 1 - c) % 2) * rows, rows)],
            dg.at[c, r, :, pl.ds(h * ff, ff)],
            load_sem.at[b, h],
        )

    def cols(t):
        return pl.ds(pl.multiple_of(t * ct, ct), ct)

    def own_load(src, t, slot):
        return pltpu.make_async_copy(src.at[:, cols(t)], ag.at[slot, 1, 0], own_sem.at[slot])

    def hop(slot, q, m):
        return remote(
            ag.at[slot, 1, q], ag.at[slot, 1, q + m], ag_send.at[slot, q + m], ag_recv.at[slot, q + m], flip(me, 2 * m)
        )

    def share(slot):
        return remote(ag.at[slot, 1], ag.at[slot, 0], ag_send.at[slot, 0], ag_recv.at[slot, 0], flip(me, 1))

    def gather_step(src, first, i):
        @pl.when((i >= 0) & (i < tiles))
        def _():
            g = i + first
            slot = g % NS
            own_load(src, i, slot).wait()

            @pl.when(g >= NS)
            def _():
                take(credit_a)

            hop(slot, 0, axes(g)[0]).start()

            @pl.when(i + 1 < tiles)
            def _():
                own_load(src, i + 1, (g + 1) % NS).start()

        t2 = i - A1

        @pl.when((t2 >= 0) & (t2 < tiles))
        def _():
            g = t2 + first
            slot = g % NS
            a, b, c = axes(g)
            hop(slot, 0, a).wait_recv()
            hop(slot, 0, b).start()
            hop(slot, a, b).start()

        t3 = i - A1 - A2

        @pl.when((t3 >= 0) & (t3 < tiles))
        def _():
            g = t3 + first
            slot = g % NS
            a, b, c = axes(g)
            hop(slot, 0, b).wait_recv()
            hop(slot, a, b).wait_recv()
            for q in (0, a, b, a + b):
                hop(slot, q, c).start()

        t4 = i - A1 - A2 - A3

        @pl.when((t4 >= 0) & (t4 < tiles))
        def _():
            g = t4 + first
            slot = g % NS
            a, b, c = axes(g)
            for q in (0, a, b, a + b):
                hop(slot, q, c).wait_recv()
            share(slot).start()

    def release(g, last):
        slot = g % NS
        a, b, c = axes(g)
        hop(slot, 0, a).wait_send()
        for q in (0, a):
            hop(slot, q, b).wait_send()
        for q in (0, a, b, a + b):
            hop(slot, q, c).wait_send()
        share(slot).wait_send()

        @pl.when(g < last)
        def _():
            give(credit_a)

    def load_wd(t):
        return pltpu.make_async_copy(wd_hbm.at[:, cols(t)], wd.at[t % 2], wd_sem.at[t % 2])

    def load_w(t):
        return [
            pltpu.make_async_copy(
                s.at[pl.ds(pl.multiple_of(t * ct, ct), ct)], w.at[t % 2, :, pl.ds(h * ff, ff)], w_sem.at[t % 2, h]
            )
            for h, s in ((0, wg_hbm), (1, wu_hbm))
        ]

    def store_dwd(t):
        return pltpu.make_async_copy(dwd.at[t % 2], dwd_hbm.at[:, cols(t)], dwd_sem.at[t % 2])

    own_load(dy_hbm, 0, 0).start()

    def start_rows(b, _):
        load_rows(b, 0).start()
        load_rows(b, 1).start()
        return 0

    lax.fori_loop(0, 16, start_rows, 0)
    load_wd(0).start()
    pl.semaphore_wait(barrier, 4)

    def hidden_block(b):
        c, r = b // 8, b % 8
        load_rows(b, 0).wait()
        load_rows(b, 1).wait()
        for n in range(nf):
            g = dg[c, r, :, n * ct : (n + 1) * ct].astype(F32)
            u = dg[c, r, :, ff + n * ct : ff + (n + 1) * ct].astype(F32)
            hid[pl.ds(pl.multiple_of(b * rows, rows), rows), n * ct : (n + 1) * ct] = (g * jax.nn.sigmoid(g) * u).astype(BF16)
            acc[c, r, :, n * ct : (n + 1) * ct] = jnp.zeros((rows, ct), F32)

    def fill(i, _):
        gather_step(dy_hbm, 0, i)
        per = 16 // LAG_A
        for e in range(per):
            hidden_block(i * per + e)
        return 0

    lax.fori_loop(0, LAG_A, fill, 0)

    def step_a(t, _):
        gather_step(dy_hbm, 0, t + LAG_A)
        slot = t % NS

        @pl.when(t + 1 < tiles)
        def _():
            load_wd(t + 1).start()

        load_wd(t).wait()
        share(slot).wait_recv()
        for c in range(2):
            block = ag[slot, c].reshape(half, ct)
            for n in range(nf):
                part = lax.dot_general(
                    block, wd[t % 2, n * ct : (n + 1) * ct, :], NT, preferred_element_type=F32
                )
                acc[c, :, :, n * ct : (n + 1) * ct] += part.reshape(8, rows, ct)

        @pl.when(t >= 2)
        def _():
            store_dwd(t - 2).wait()

        piece = ff // 2
        for n in range(2):
            dwd[t % 2, n * piece : (n + 1) * piece, :] = lax.dot_general(
                hid[:, n * piece : (n + 1) * piece], ag[slot].reshape(2 * half, ct), TN, preferred_element_type=F32
            ).astype(BF16)
        release(t, 2 * tiles - NS)
        store_dwd(t).start()
        return 0

    lax.fori_loop(0, tiles, step_a, 0)

    give(credit_b, NR)
    for c in load_w(0):
        c.start()
    own_load(x_hbm, 0, tiles % NS).start()

    def d_act(b, _):
        @pl.when(b % 4 == 0)
        def _():
            gather_step(x_hbm, tiles, b // 4)

        c, r = b // 8, b % 8
        for n in range(nf):
            lo, hi = slice(n * ct, (n + 1) * ct), slice(ff + n * ct, ff + (n + 1) * ct)
            g, u, d = dg[c, r, :, lo].astype(F32), dg[c, r, :, hi].astype(F32), acc[c, r, :, lo]
            s = jax.nn.sigmoid(g)
            dg[c, r, :, lo] = (d * u * (s + g * s * (1.0 - s))).astype(BF16)
            dg[c, r, :, hi] = (d * (g * s)).astype(BF16)
        return 0

    lax.fori_loop(0, 16, d_act, 0)
    for t in (tiles - 2, tiles - 1):
        store_dwd(t).wait()

    def place(t):
        k = t % NR
        return k // nf, pl.ds(pl.multiple_of((k % nf) * ct, ct), ct)

    def c0(t):
        c, n = place(t)
        return remote(s0.at[t % SND], hid.at[pl.ds(pl.multiple_of(c * half, half), half), n], s0_sem.at[t % SND], r0_sem.at[t % NR], flip(me, 1))

    def c1(t):
        return remote(
            s1.at[t % SND], r1.at[t % NR], s1_sem.at[t % SND], r1_sem.at[t % NR], flip(me, 2 * axes(t)[0])
        )

    def c2(t):
        return remote(
            s2.at[t % SND], r2.at[t % NR], s2_sem.at[t % SND], r2_sem.at[t % NR], flip(me, 2 * axes(t)[1])
        )

    def c3(t):
        return remote(
            s3.at[t % SND], r3.at[t % NR], s3_sem.at[t % SND], r3_sem.at[t % NR], flip(me, 2 * axes(t)[2])
        )

    def chip_sum(t, r):
        c, n = place(t)
        return acc[c, r, :, n] + hid[pl.ds(pl.multiple_of(c * half + r * rows, rows), rows), n].astype(F32)

    def store_dw(t):
        return [
            pltpu.make_async_copy(
                w.at[t % 2, :, pl.ds(h * ff, ff)], o.at[pl.ds(pl.multiple_of(t * ct, ct), ct)], out_sem.at[t % 2, h]
            )
            for h, o in ((0, dwg_hbm), (1, dwu_hbm))
        ]

    def step_b(i, _):
        @pl.when(i < tiles)
        def _():
            @pl.when(i + 1 < tiles)
            def _():
                for c in load_w(i + 1):
                    c.start()

            for c in load_w(i):
                c.wait()

            @pl.when(i >= SND)
            def _():
                c0(i - SND).wait_send()

            part = lax.dot_general(dg[0].reshape(half, 2 * ff), w[i % 2], NT, preferred_element_type=F32)
            s0[i % SND] = part.astype(BF16)

        t1, t2, t3, t4 = i - 1, i - 1 - B1, i - 1 - B1 - B2, i - LAG_B

        @pl.when((t1 >= 0) & (t1 < tiles))
        def _():
            @pl.when(t1 >= SND)
            def _():
                c1(t1 - SND).wait_send()

            c0(t1).wait_recv()
            a, b, c = axes(t1)
            for q, r in enumerate((a, a + c, a + b, a + b + c)):
                s1[t1 % SND, q] = chip_sum(t1, r).astype(BF16)

        @pl.when((t2 >= 0) & (t2 < tiles))
        def _():
            @pl.when(t2 >= SND)
            def _():
                c2(t2 - SND).wait_send()

            c1(t2).wait_recv()
            a, b, c = axes(t2)
            for q, r in enumerate((b, b + c)):
                s2[t2 % SND, q] = (chip_sum(t2, r) + r1[t2 % NR, 2 + q].astype(F32)).astype(BF16)

        @pl.when((t3 >= 0) & (t3 < tiles))
        def _():
            @pl.when(t3 >= SND)
            def _():
                c3(t3 - SND).wait_send()

            c2(t3).wait_recv()
            a, b, c = axes(t3)
            s3[t3 % SND] = (
                chip_sum(t3, c) + r1[t3 % NR, 1].astype(F32) + r2[t3 % NR, 1].astype(F32)
            ).astype(BF16)

        @pl.when((t4 >= 0) & (t4 < tiles))
        def _():
            c3(t4).wait_recv()
            total = chip_sum(t4, 0) + r1[t4 % NR, 0].astype(F32) + r2[t4 % NR, 0].astype(F32)
            dx_ref[:, cols(t4)] = (total + r3[t4 % NR].astype(F32)).astype(BF16)

            @pl.when(t4 < tiles - NR)
            def _():
                give(credit_b)

        @pl.when(i < tiles)
        def _():
            take(credit_b)
            c0(i).start()

        for copy, t in ((c3, t3), (c2, t2), (c1, t1)):
            @pl.when((t >= 0) & (t < tiles))
            def _():
                copy(t).start()

        k = jnp.where(i < tiles, i + 4, i - tiles + LAG_A)

        @pl.when((i < LAG_A - 4) | (i >= tiles))
        def _():
            gather_step(x_hbm, tiles, k)

        @pl.when(i < tiles)
        def _():
            c, n = place(i)
            part = lax.dot_general(dg[1].reshape(half, 2 * ff), w[i % 2], NT, preferred_element_type=F32)
            acc[c, :, :, n] = part.reshape(8, rows, ct)

        t = i - tiles

        @pl.when(t >= 0)
        def _():
            g = t + tiles

            @pl.when(t >= 2)
            def _():
                for c in store_dw(t - 2):
                    c.wait()

            share(g % NS).wait_recv()
            block = ag[g % NS].reshape(2 * half, ct)
            for h in range(2):
                w[t % 2, :, h * ff : (h + 1) * ff] = lax.dot_general(
                    block, dg[:, :, :, h * ff : (h + 1) * ff].reshape(2 * half, ff), TN, preferred_element_type=F32
                ).astype(BF16)
            release(g, 2 * tiles - NS)
            for c in store_dw(t):
                c.start()

        return 0

    lax.fori_loop(0, 2 * tiles, step_b, 0)
    for t in range(tiles - SND, tiles):
        for c in (c0, c1, c2, c3):
            c(t).wait_send()
    for t in (tiles - 2, tiles - 1):
        for c in store_dw(t):
            c.wait()


def mlp_backward(x, dy, gate, up, w_gate, w_up, w_down, ct=256):
    rows, d = x.shape
    n, ff = gate.shape
    tiles, nf = d // ct, ff // ct
    assert n == 16 * rows and 2 * nf == NR and tiles >= NS
    anywhere = pl.BlockSpec(memory_space=pl.ANY)
    dma, vmem = pltpu.SemaphoreType.DMA, pltpu.VMEM
    return pl.pallas_call(
        functools.partial(kernel, tiles),
        out_shape=[
            jax.ShapeDtypeStruct((rows, d), BF16),
            jax.ShapeDtypeStruct((d, ff), BF16),
            jax.ShapeDtypeStruct((d, ff), BF16),
            jax.ShapeDtypeStruct((ff, d), BF16),
        ],
        in_specs=[anywhere] * 7,
        out_specs=[pl.BlockSpec(memory_space=vmem)] + [anywhere] * 3,
        scratch_shapes=[
            vmem((NS, 2, 8, rows, ct), BF16),
            vmem((2, 8, rows, ff), F32),
            vmem((16 * rows, ff), BF16),
            vmem((2, 8, rows, 2 * ff), BF16),
            vmem((2, ct, 2 * ff), BF16),
            vmem((2, ff, ct), BF16),
            vmem((2, ff, ct), BF16),
            vmem((SND, 8 * rows, ct), BF16),
            vmem((SND, 4, rows, ct), BF16),
            vmem((SND, 2, rows, ct), BF16),
            vmem((SND, rows, ct), BF16),
            vmem((NR, 4, rows, ct), BF16),
            vmem((NR, 2, rows, ct), BF16),
            vmem((NR, rows, ct), BF16),
            dma((NS, 8)), dma((NS, 8)), dma((NS,)), dma((16, 2)), dma((2, 2)), dma((2,)), dma((2,)), dma((2, 2)),
            dma((SND,)), dma((SND,)), dma((SND,)), dma((SND,)), dma((NR,)), dma((NR,)), dma((NR,)), dma((NR,)),
            pltpu.SemaphoreType.REGULAR((4,)), pltpu.SemaphoreType.REGULAR((4,)),
        ],
        compiler_params=pltpu.CompilerParams(collective_id=0, has_side_effects=True, vmem_limit_bytes=67000000),
        cost_estimate=pl.CostEstimate(flops=12 * n * ff * d, bytes_accessed=12 * ff * d, transcendentals=0),
    )(x, dy, gate, up, w_gate, w_up, w_down)


def solution(mesh):
    rows, cols = P(("dp", "tp"), None), P("dp", "tp")
    return jax.shard_map(
        mlp_backward,
        mesh=mesh,
        in_specs=(rows, rows, cols, cols, P(None, "tp"), P(None, "tp"), P("tp", None)),
        out_specs=(rows, cols, cols, P(("dp", "tp"), None)),
        check_vma=False,
    )
```
